32 devices in a mesh: irrep: 4 (over z), occ: 4 (over y, core), vir: 2 (over x).
Axes of the slice: x: 2, y: 2, z: 4, core: 2. Of those that a mesh axis runs over, the one named last changes fastest.
Arguments:
- amplitudes: bfloat16 [8, 320, 12288], P('irrep', None, ('occ', 'vir')), may hold values from -6 to 6
- ladder_ints: bfloat16 [8, 12288, 12288], P('irrep', ('occ', 'vir')), may hold values from -0.078125 to 0.078125
- hole_ints: bfloat16 [8, 320, 320], P('irrep'), may hold values from -0.3125 to 0.3125
- occ_energy: float32 [8, 320], P('irrep'), may hold values from -3 to -0.5
- vir_energy: float32 [8, 12288], P('irrep', ('occ', 'vir')), may hold values from 0.5 to 3
- occ_pairs: int32 [8], replicated, may hold values from 160 to 320, as said below
- vir_pairs: int32 [8], replicated, may hold values from 6144 to 12288, as said below
Outputs:
- updated: bfloat16 [8, 320, 12288], P('irrep', None, ('occ', 'vir'))
- residual_norm: float32 [8], P('irrep')
The draws below stay inside these ranges and needn't reach their ends.
Inputs may be any that keep to these rules, and one draw needn't show every extreme that they name: `occ_pairs`: some block has exactly 320 live occupied pairs in every draw. `vir_pairs`: some block has exactly 12288 live virtual pairs in every draw.
All inputs are finite; a program needn't handle non-finite values.
Results may differ from the reference program's by a relative error of at most 0.001.
Values may be sent and summed in bfloat16 or wider, within the bound.
A program may use at most 192 MiB of HBM per device.

```python
import jax
import jax.numpy as jnp

NB = 8
OP = 320
VP = 12288


def draw_occ_pairs(key, part):
    first_key, second_key = jax.random.split(jax.random.fold_in(key, 11))
    values = jax.random.randint(first_key, (NB,), OP // 2, OP + 1)
    chosen = jax.random.randint(second_key, (), 0, NB)
    return jnp.where(jnp.arange(NB) == chosen, OP, values).astype(jnp.int32)


def draw_vir_pairs(key, part):
    first_key, second_key = jax.random.split(jax.random.fold_in(key, 23))
    values = jax.random.randint(first_key, (NB,), VP // 2, VP + 1)
    chosen = jax.random.randint(second_key, (), 0, NB)
    return jnp.where(jnp.arange(NB) == chosen, VP, values).astype(jnp.int32)


def with_spikes(drawn, stream_key, source, target, shards_of, factor):
    def block_of(dim):
        return (jnp.arange(drawn.shape[dim]) // (drawn.shape[dim] // shards_of)).reshape((-1,) + (1,) * (drawn.ndim - 1 - dim))

    near = jax.random.permutation(stream_key, shards_of)[block_of(target)]
    second = (block_of(target) + shards_of // 2) % shards_of
    return jnp.where((block_of(source) == near) | (block_of(source) == second), factor * drawn, drawn)


def shard_levels(stream_key, shape, pieces, low, largest):
    def one(position, blocks):
        steps = jax.random.uniform(jax.random.fold_in(jax.random.fold_in(stream_key, 6), position), (blocks,), jnp.float32, low / len(pieces), largest / len(pieces))
        return jnp.repeat(jnp.exp(steps), shape[position] // blocks).reshape((-1,) + (1,) * (len(shape) - position - 1))

    gain = one(*pieces[0])
    for cut in pieces[1:]:
        gain = gain * one(*cut)
    return gain


def centred(stream_key, dims, scale, bound, cuts=(), kind=jnp.bfloat16):
    gain = shard_levels(stream_key, dims, cuts, -0.22, 0.18) if cuts else 1.0
    result = jax.random.normal(stream_key, dims, jnp.float32) * scale * gain
    return jnp.minimum(jnp.maximum(result, -bound), bound).astype(kind)


def heavy_noise(own_key, shape, deviation, bound, shards, heavy, kind=jnp.bfloat16):
    entries = deviation * jax.random.normal(own_key, shape, jnp.float32)
    if shards:
        entries = entries * shard_levels(own_key, shape, shards, -0.22, 0.18)
    return jnp.clip(with_spikes(entries, jax.random.fold_in(own_key, 3), *heavy), -bound, bound).astype(kind)


def setup_inputs(seed: int = 0) -> dict:
    splits = jax.random.split(jax.random.key(seed), 8)
    amplitudes = centred(splits[0], (NB, OP, VP), 1.0, 6.0, ((0, 4), (2, 8)))
    ladder_ints = heavy_noise(splits[1], (NB, VP, VP), VP ** -0.5, 0.078125, ((0, 4), (1, 8)), (1, 2, 8, 2.0))
    hole_ints = centred(splits[2], (NB, OP, OP), OP ** -0.5, 0.3125, ((0, 4),))
    occ_energy = jnp.clip(-3.0 + 2.5 * jax.random.uniform(splits[3], (NB, OP), jnp.float32) ** shard_levels(splits[3], (NB, OP), ((0, 4),), -0.2, 0.2), -3.0, -0.5)
    vir_energy = jnp.clip(0.5 + 2.5 * jax.random.uniform(splits[4], (NB, VP), jnp.float32) ** shard_levels(splits[4], (NB, VP), ((0, 4), (1, 8)), -0.2, 0.2), 0.5, 3.0)
    occ_pairs = draw_occ_pairs(jax.random.fold_in(splits[7], 71), 0)
    vir_pairs = draw_vir_pairs(jax.random.fold_in(splits[7], 71), 0)
    return dict(amplitudes=amplitudes, ladder_ints=ladder_ints, hole_ints=hole_ints, occ_energy=occ_energy, vir_energy=vir_energy, occ_pairs=occ_pairs, vir_pairs=vir_pairs)


LEVEL_SHIFT = 0.5
EPSILON = 1e-06

def reference(amplitudes, ladder_ints, hole_ints, occ_energy, vir_energy, occ_pairs, vir_pairs):
    row_index = jnp.arange(OP, dtype=jnp.int32)
    col_index = jnp.arange(VP, dtype=jnp.int32)
    results = []
    norms = []
    for block in range(NB):
        keep_mask = (row_index[:, None] < occ_pairs[block]) & (col_index[None, :] < vir_pairs[block])
        masked = jnp.where(keep_mask, amplitudes[block], jnp.zeros((), amplitudes.dtype))
        ladder_term = jnp.dot(masked, ladder_ints[block], preferred_element_type=jnp.float32)
        hole_term = jnp.dot(hole_ints[block], masked, preferred_element_type=jnp.float32)
        wide = masked.astype(jnp.float32)
        denominator = vir_energy[block][None, :] - occ_energy[block][:, None]
        residual = jnp.where(keep_mask, ladder_term + hole_term + denominator * wide, jnp.zeros((), jnp.float32))
        updated = wide - residual / (denominator + LEVEL_SHIFT)
        pair_count = (occ_pairs[block] * vir_pairs[block]).astype(jnp.float32)
        results.append(updated.astype(jnp.bfloat16))
        norms.append(jnp.sqrt(jnp.sum(residual * residual) / pair_count + EPSILON))
    return (jnp.stack(results), jnp.stack(norms))
```

```python
import functools

import jax
import jax.numpy as jnp
from jax import lax
from jax.experimental import pallas as pl
from jax.experimental.pallas import tpu as pltpu
from jax.sharding import PartitionSpec as P

LEVEL_SHIFT = 0.5
EPSILON = 1e-06
GRID_STEPS = 256.0
TOP = 32767.0
CODE_ROWS = 16
SLOTS = ("occ", "vir")


def encode(value, out_ref):
    rows, cols = value.shape
    largest = jnp.max(jnp.abs(value), axis=0, keepdims=True)
    code = jnp.ceil(jnp.log2(jnp.maximum(largest, 1e-30)) * GRID_STEPS) + 1.0
    scaled = value * (jnp.exp2(code * (-1.0 / GRID_STEPS)) * TOP)
    out_ref[0:rows, :] = jnp.round(scaled).astype(jnp.int32).astype(jnp.int16)
    out_ref[rows : rows + CODE_ROWS, :] = (
        jnp.broadcast_to(code, (CODE_ROWS, cols)).astype(jnp.int32).astype(jnp.int16)
    )


def decode(in_ref):
    rows = in_ref.shape[0] - CODE_ROWS
    codes = in_ref[rows : rows + CODE_ROWS, :].astype(jnp.int32).astype(jnp.float32)
    scale = jnp.exp2(codes[0:1, :] * (1.0 / GRID_STEPS)) * (1.0 / TOP)
    return in_ref[0:rows, :].astype(jnp.int32).astype(jnp.float32) * scale


def ladder_kernel(received, coded, slot_ref, amp_ref, ladder_ref, *refs):
    out_ref = refs[-1]
    value = jnp.dot(amp_ref[0], ladder_ref[0], preferred_element_type=jnp.float32)
    for ref in refs[:received]:
        value = value + decode(ref)
    if coded:
        encode(value, out_ref)
    else:
        out_ref[...] = value


def tile_of(cols):
    return next(size for size in (768, 512, 384, 256, 128) if cols % size == 0)


def ladder_call(block, slot, masked, ladder, received, coded):
    _, rows, cols = masked.shape
    tile = tile_of(cols)
    steps = cols // tile
    out_rows, out_type = (rows + CODE_ROWS, jnp.int16) if coded else (rows, jnp.float32)
    return pl.pallas_call(
        functools.partial(ladder_kernel, len(received), coded),
        grid_spec=pltpu.PrefetchScalarGridSpec(
            num_scalar_prefetch=1,
            grid=(steps,),
            in_specs=[
                pl.BlockSpec((1, rows, cols), lambda j, slot: (block, 0, 0)),
                pl.BlockSpec((1, cols, tile), lambda j, slot: (block, 0, slot[0] * steps + j)),
            ]
            + [pl.BlockSpec((rows + CODE_ROWS, tile), lambda j, slot: (0, j))] * len(received),
            out_specs=pl.BlockSpec((out_rows, tile), lambda j, slot: (0, j)),
        ),
        out_shape=jax.ShapeDtypeStruct((out_rows, cols), out_type),
        cost_estimate=pl.CostEstimate(
            flops=2 * rows * cols * cols,
            bytes_accessed=2 * cols * cols + 4 * rows * cols * (1 + len(received)),
            transcendentals=0,
        ),
        name="ladder",
    )(slot.reshape(1), masked, ladder, *received)


def join_kernel(total_ref, *refs):
    value = total_ref[...]
    for ref in refs[:-1]:
        value = value + decode(ref)
    encode(value, refs[-1])


def join_call(total, received):
    rows, cols = total.shape
    tile = tile_of(cols)
    coded = pl.BlockSpec((rows + CODE_ROWS, tile), lambda j: (0, j))
    return pl.pallas_call(
        join_kernel,
        grid=(cols // tile,),
        in_specs=[pl.BlockSpec((rows, tile), lambda j: (0, j))] + [coded] * len(received),
        out_specs=coded,
        out_shape=jax.ShapeDtypeStruct((rows + CODE_ROWS, cols), jnp.int16),
        cost_estimate=pl.CostEstimate(
            flops=8 * rows * cols, bytes_accessed=(6 + 2 * len(received)) * rows * cols, transcendentals=0
        ),
        name="join",
    )(total, *received)


def final_kernel(blocks, parts, start_ref, occ_ref, vir_ref, amp_ref, hole_ref, occ_energy_ref, vir_energy_ref, *refs):
    out_ref, square_ref = refs[-2], refs[-1]
    rows, tile = out_ref.shape[1:]
    step = pl.program_id(0)
    column = start_ref[0] + step * tile + lax.broadcasted_iota(jnp.int32, (rows, tile), 1)
    row = lax.broadcasted_iota(jnp.int32, (rows, tile), 0)
    for block in range(blocks):
        mine = refs[block * parts : (block + 1) * parts]
        value = mine[0][...]
        for ref in mine[1:]:
            value = value + decode(ref)
        amp = amp_ref[block]
        value = value + jnp.dot(hole_ref[block], amp, preferred_element_type=jnp.float32)
        wide = amp.astype(jnp.float32)
        denominator = vir_energy_ref[block] - occ_energy_ref[block]
        keep = (row < occ_ref[block]) & (column < vir_ref[block])
        residual = jnp.where(keep, value + denominator * wide, 0.0)
        out_ref[block] = (wide - residual / (denominator + LEVEL_SHIFT)).astype(jnp.bfloat16)
        squares = jnp.sum((residual * residual).reshape(rows // 8, 8, tile), axis=0)
        squares = jnp.broadcast_to(jnp.sum(squares), (8, 128))

        @pl.when(step == 0)
        def _():
            square_ref[block] = squares

        @pl.when(step != 0)
        def _():
            square_ref[block] += squares


def final_call(start, occ_here, vir_here, masked, hole, occ_energy, vir_energy, operands):
    blocks, rows, cols = masked.shape
    parts = len(operands[0])
    tile = 512 if cols % 512 == 0 else tile_of(cols)
    total = pl.BlockSpec((rows, tile), lambda j, *_: (0, j))
    coded = pl.BlockSpec((rows + CODE_ROWS, tile), lambda j, *_: (0, j))
    return pl.pallas_call(
        functools.partial(final_kernel, blocks, parts),
        grid_spec=pltpu.PrefetchScalarGridSpec(
            num_scalar_prefetch=3,
            grid=(cols // tile,),
            in_specs=[
                pl.BlockSpec((blocks, rows, tile), lambda j, *_: (0, 0, j)),
                pl.BlockSpec((blocks, rows, rows), lambda j, *_: (0, 0, 0)),
                pl.BlockSpec((blocks, rows, 1), lambda j, *_: (0, 0, 0)),
                pl.BlockSpec((blocks, 1, tile), lambda j, *_: (0, 0, j)),
            ]
            + ([total] + [coded] * (parts - 1)) * blocks,
            out_specs=[
                pl.BlockSpec((blocks, rows, tile), lambda j, *_: (0, 0, j)),
                pl.BlockSpec((blocks, 8, 128), lambda j, *_: (0, 0, 0)),
            ],
        ),
        out_shape=[
            jax.ShapeDtypeStruct((blocks, rows, cols), jnp.bfloat16),
            jax.ShapeDtypeStruct((blocks, 8, 128), jnp.float32),
        ],
        cost_estimate=pl.CostEstimate(
            flops=2 * blocks * rows * rows * cols, bytes_accessed=12 * blocks * rows * cols, transcendentals=0
        ),
        name="final",
    )(
        start.reshape(1), occ_here, vir_here, masked, hole,
        occ_energy[:, :, None], vir_energy[:, None, :], *[x for group in operands for x in group],
    )


def table_lookup(table, block_ids):
    entries = table.shape[0]
    match = jnp.arange(entries, dtype=jnp.int32)[None, :] == block_ids[:, None]
    return jnp.sum(jnp.where(match, table[None, :], 0), axis=1)


def body(amplitudes, ladder_ints, hole_ints, occ_energy, vir_energy, occ_pairs, vir_pairs):
    blocks, rows, cols = amplitudes.shape
    occ_size, vir_size = lax.axis_size("occ"), lax.axis_size("vir")
    slots = occ_size * vir_size
    block_ids = lax.axis_index("irrep") * blocks + jnp.arange(blocks, dtype=jnp.int32)
    slot = lax.axis_index("occ") * vir_size + lax.axis_index("vir")
    start = slot * cols
    occ_here = table_lookup(occ_pairs, block_ids)
    vir_here = table_lookup(vir_pairs, block_ids)
    row = jnp.arange(rows, dtype=jnp.int32)
    column = start + jnp.arange(cols, dtype=jnp.int32)
    keep = (row[None, :, None] < occ_here[:, None, None]) & (column[None, None, :] < vir_here[:, None, None])
    masked = jnp.where(keep, amplitudes, jnp.zeros((), amplitudes.dtype))

    core = vir_size if occ_size > vir_size else 1
    bits = [1 << i for i in range(slots.bit_length() - 1) if 1 << i != core]

    def exchange(array, bit):
        return lax.ppermute(array, SLOTS, [(s, s ^ bit) for s in range(slots)])

    orders = [bits if block % 2 == 0 else bits[::-1] for block in range(blocks)]
    arrived = [{} for _ in range(blocks)]
    for rank in range((1 << len(bits)) - 1, -1, -1):
        chosen = [i for i in range(len(bits)) if rank >> (len(bits) - 1 - i) & 1]
        flips = [sum(order[i] for i in chosen) for order in orders]
        firsts = [ladder_call(b, slot ^ (flips[b] | core), masked, ladder_ints, [], True) for b in range(blocks)]
        firsts = [exchange(first, core) for first in firsts]
        for b in range(blocks):
            order, got = orders[b], arrived[b].get(flips[b], [])
            direct = bool(chosen) and not got
            total = ladder_call(b, slot ^ flips[b], masked, ladder_ints, [firsts[b]], direct)
            if not chosen:
                arrived[b][0] = [total] + got
                continue
            packed = total if direct else join_call(total, got)
            bit = order[chosen[0]]
            arrived[b].setdefault(flips[b] ^ bit, []).append(exchange(packed, bit))
    updated, squares = final_call(
        start, occ_here, vir_here, masked, hole_ints, occ_energy, vir_energy, [arrived[b][0] for b in range(blocks)]
    )
    summed_squares = lax.psum(squares[:, 0, 0], SLOTS)
    pair_count = (occ_here * vir_here).astype(jnp.float32)
    return updated, jnp.sqrt(summed_squares / pair_count + EPSILON)


def solution(mesh):
    in_specs = (
        P("irrep", None, SLOTS),
        P("irrep", SLOTS, None),
        P("irrep", None, None),
        P("irrep", None),
        P("irrep", SLOTS),
        P(),
        P(),
    )
    out_specs = (P("irrep", None, SLOTS), P("irrep"))
    return jax.shard_map(body, mesh=mesh, in_specs=in_specs, out_specs=out_specs, check_vma=False)
```
